32 devices in a mesh: dp: 16 (over z, y, x), mp: 2 (over core).
Axes of the slice: x: 2, y: 2, z: 4, core: 2. Of those that a mesh axis runs over, the one named last changes fastest.
Arguments:
- residual_input: bfloat16 [4096, 5120], P('dp', 'mp'), may hold values from -6 to 6
- cotangent: bfloat16 [4096, 5120], P('dp', 'mp'), may hold values from -0.6 to 0.6
- lengths: int32 [16], P('dp'), may hold values from 64 to 256
- norm_gain_vector: bfloat16 [5120], replicated, may hold values from 0.5 to 1.5
- gate_projection_weight: bfloat16 [5120, 6912], P('dp', 'mp'), may hold values from -0.078125 to 0.078125
- up_projection_weight: bfloat16 [5120, 6912], P('dp', 'mp'), may hold values from -0.078125 to 0.078125
- down_projection_weight: bfloat16 [5120, 6912], P('dp', 'mp'), may hold values from -0.078125 to 0.078125
- up_adapter_first: bfloat16 [5120, 16], replicated, may hold values from -0.078125 to 0.078125
- up_adapter_second: bfloat16 [16, 6912], P(None, 'mp'), may hold values from -0.29882812 to 0.29882812
- down_adapter_first: bfloat16 [6912, 16], P('mp'), may hold values from -0.078125 to 0.078125
- down_adapter_second: bfloat16 [16, 5120], replicated, may hold values from -0.29882812 to 0.29882812
Outputs:
- up_first_gradient: float32 [5120, 16], P('dp')
- up_second_gradient: float32 [16, 6912], P(None, ('mp', 'dp'))
- down_first_gradient: float32 [6912, 16], P(('mp', 'dp'))
- down_second_gradient: float32 [16, 5120], P(None, 'dp')
The draws below stay inside these ranges and needn't reach their ends.
All inputs are finite; a program needn't handle non-finite values.
Results may differ from the reference program's by a relative error of at most 0.0061.
Values may be sent and summed in bfloat16 or wider, within the bound.
No kernel may reach another device: no remote copies, remote signals or barrier semaphores. Data moves between devices by JAX's collectives and lax.ppermute only.
A program may use at most 192 MiB of HBM per device.

```python
import math
import jax
import jax.numpy as jnp
from jax import lax

MODEL_WIDTH = 5120
HIDDEN_SHARD = 6912
ADAPTER_RANK = 16
SEQ = 256
BATCH = 16
TOKENS = 4096


def draw_cotangent(key, part):
    row_key = jax.random.fold_in(key, 11)
    value_key = jax.random.fold_in(key, 23)
    spread = jnp.exp(jax.random.uniform(row_key, (BATCH, 1, 1), jnp.float32, 0.0, math.log(10.0)))
    values = jnp.clip(jax.random.normal(value_key, (BATCH, SEQ, MODEL_WIDTH), jnp.float32), -6.0, 6.0)
    return (0.01 * spread * values).reshape(BATCH * SEQ, MODEL_WIDTH).astype(jnp.bfloat16)


def touch_ends(result, key, smallest, top_value):
    shape = result.shape
    place = [jax.random.randint(jax.random.fold_in(key, axis), (), 0, shape[axis]) for axis in range(len(shape))]
    result = result.at[tuple(place)].set(smallest)
    longest = shape.index(max(shape))
    place[longest] = (place[longest] + 1) % shape[longest]
    return result.at[tuple(place)].set(top_value)


def level_of(own_key, dims, split, smallest, high):
    level = 1.0
    for axis_at, parts in split:
        steps = jax.random.uniform(jax.random.fold_in(jax.random.fold_in(own_key, 6), axis_at), (parts,), jnp.float32, smallest / len(split), high / len(split))
        level = level * jnp.repeat(jnp.exp(steps), dims[axis_at] // parts).reshape((-1,) + (1,) * (len(dims) - 1 - axis_at))
    return level


def gaussian(rng, dims, scale, bound, pieces=(), kind=jnp.bfloat16):
    factor_of = level_of(rng, dims, pieces, -0.22, 0.18) if pieces else 1.0
    entries = jax.random.normal(rng, dims, jnp.float32) * scale * factor_of
    return jnp.minimum(jnp.maximum(entries, -bound), bound).astype(kind)


def setup_inputs(seed: int = 0) -> dict:
    seeds = jax.random.split(jax.random.key(seed), 12)
    residual_input = gaussian(seeds[0], (TOKENS, MODEL_WIDTH), 1.0, 6.0, ((0, 16), (1, 2)))
    cotangent = draw_cotangent(jax.random.fold_in(seeds[11], 71), 0)
    lengths = touch_ends(jax.random.randint(seeds[2], (BATCH,), SEQ // 4, SEQ + 1), jax.random.fold_in(seeds[2], 1), SEQ // 4, SEQ).astype(jnp.int32)
    norm_gain_vector = jnp.clip(1.0 + 0.1 * jax.random.normal(seeds[3], (MODEL_WIDTH,), jnp.float32), 0.5, 1.5).astype(jnp.bfloat16)
    gate_projection_weight = gaussian(seeds[4], (MODEL_WIDTH, HIDDEN_SHARD), MODEL_WIDTH ** -0.5, 0.078125, ((0, 16), (1, 2)))
    up_projection_weight = gaussian(seeds[5], (MODEL_WIDTH, HIDDEN_SHARD), MODEL_WIDTH ** -0.5, 0.078125, ((0, 16), (1, 2)))
    down_projection_weight = gaussian(seeds[6], (MODEL_WIDTH, HIDDEN_SHARD), HIDDEN_SHARD ** -0.5, 0.078125, ((0, 16), (1, 2)))
    up_adapter_first = gaussian(seeds[7], (MODEL_WIDTH, ADAPTER_RANK), MODEL_WIDTH ** -0.5, 0.078125)
    up_adapter_second = gaussian(seeds[8], (ADAPTER_RANK, HIDDEN_SHARD), 0.05, 0.29882812, ((1, 2),))
    down_adapter_first = gaussian(seeds[9], (HIDDEN_SHARD, ADAPTER_RANK), HIDDEN_SHARD ** -0.5, 0.078125, ((0, 2),))
    down_adapter_second = gaussian(seeds[10], (ADAPTER_RANK, MODEL_WIDTH), 0.05, 0.29882812)
    return {"residual_input": residual_input, "cotangent": cotangent, "lengths": lengths, "norm_gain_vector": norm_gain_vector, "gate_projection_weight": gate_projection_weight, "up_projection_weight": up_projection_weight, "down_projection_weight": down_projection_weight, "up_adapter_first": up_adapter_first, "up_adapter_second": up_adapter_second, "down_adapter_first": down_adapter_first, "down_adapter_second": down_adapter_second}


norm_eps = 1e-06
adapter_scale = 2.0
clip_coefficient = 0.005

def reference(residual_input, cotangent, lengths, norm_gain_vector, gate_projection_weight, up_projection_weight, down_projection_weight, up_adapter_first, up_adapter_second, down_adapter_first, down_adapter_second):
    single_float = jnp.float32
    half_precision = jnp.bfloat16
    clip_limit = clip_coefficient * math.sqrt(2.0 * ADAPTER_RANK * (MODEL_WIDTH + HIDDEN_SHARD))
    positions = jnp.arange(SEQ, dtype=jnp.int32)
    live = (positions[None, :] < lengths[:, None]).astype(single_float).reshape(TOKENS, 1)
    output_gradient = (cotangent.astype(single_float) * live).astype(half_precision)
    wide = residual_input.astype(single_float)
    inverse = lax.rsqrt(lax.optimization_barrier(jnp.mean(wide * wide, axis=1, keepdims=True)) + norm_eps)
    normalized_input = (wide * inverse * norm_gain_vector.astype(single_float)).astype(half_precision)
    up_adapter_latent = jnp.dot(normalized_input, up_adapter_first, preferred_element_type=single_float).astype(half_precision)
    gate = jnp.dot(normalized_input, gate_projection_weight, preferred_element_type=single_float)
    up_activation = jnp.dot(normalized_input, up_projection_weight, preferred_element_type=single_float) + adapter_scale * jnp.dot(up_adapter_latent, up_adapter_second, preferred_element_type=single_float)
    gate_act = jax.nn.silu(gate)
    hidden_activation = (gate_act * up_activation).astype(half_precision)
    down_adapter_latent = jnp.dot(hidden_activation, down_adapter_first, preferred_element_type=single_float).astype(half_precision)
    backward_adapter = jnp.dot(output_gradient, down_adapter_second.T, preferred_element_type=single_float).astype(half_precision)
    hidden_gradient = jnp.dot(output_gradient, down_projection_weight, preferred_element_type=single_float) + adapter_scale * jnp.dot(backward_adapter, down_adapter_first.T, preferred_element_type=single_float)
    up_gradient = (hidden_gradient * gate_act).astype(half_precision)
    up_adapter_hidden = jnp.dot(up_gradient, up_adapter_second.T, preferred_element_type=single_float).astype(half_precision)

    def split_parts(values):
        return values.astype(single_float).reshape(BATCH, SEQ, values.shape[1])
    example_down_second = adapter_scale * jnp.einsum('kox,kou->kxu', split_parts(down_adapter_latent), split_parts(output_gradient))
    example_down_first = adapter_scale * jnp.einsum('yze,yzx->yex', split_parts(hidden_activation), split_parts(backward_adapter))
    example_up_second = adapter_scale * jnp.einsum('uml,umk->ulk', split_parts(up_adapter_latent), split_parts(up_gradient))
    example_up_first = adapter_scale * jnp.einsum('mju,mjl->mul', split_parts(normalized_input), split_parts(up_adapter_hidden))
    squares = lax.optimization_barrier(jnp.sum(example_down_second * example_down_second, axis=(1, 2))) + lax.optimization_barrier(jnp.sum(example_down_first * example_down_first, axis=(1, 2)))
    squares = squares + lax.optimization_barrier(jnp.sum(example_up_second * example_up_second, axis=(1, 2))) + lax.optimization_barrier(jnp.sum(example_up_first * example_up_first, axis=(1, 2)))
    factor = jnp.minimum(1.0, clip_limit / (jnp.sqrt(squares) + 1e-06))
    up_first_gradient = jnp.einsum('b,bdr->dr', factor, example_up_first)
    up_second_gradient = jnp.einsum('b,brf->rf', factor, example_up_second)
    down_first_gradient = jnp.einsum('b,bfr->fr', factor, example_down_first)
    down_second_gradient = jnp.einsum('b,brd->rd', factor, example_down_second)
    return (up_first_gradient, up_second_gradient, down_first_gradient, down_second_gradient)
```

```python
import math

import jax
import jax.numpy as jnp
from jax import lax
from jax.sharding import Mesh, PartitionSpec as P

norm_eps = 1e-06
adapter_scale = 2.0
clip_coefficient = 0.005


def matmul(left, right):
    return jnp.dot(left, right, preferred_element_type=jnp.float32)


def contract(left, right, left_dim, right_dim):
    return lax.dot_general(
        left, right, (((left_dim,), (right_dim,)), ((), ())), preferred_element_type=jnp.float32
    )


def outer_count(dp):
    return min(r for r in range(1, dp + 1) if dp % r == 0 and r * r >= dp)


def exchange_columns(weight, r):
    o = lax.axis_index("o")
    rows, width = weight.shape[0], weight.shape[1] // r
    out = jnp.zeros((r, rows, width), weight.dtype)
    own = lax.dynamic_slice(weight, (0, o * width), (rows, width))
    out = lax.dynamic_update_slice(out, own[None], (o, 0, 0))
    for d in range(1, r):
        piece = lax.dynamic_slice(weight, (0, (o + d) % r * width), (rows, width))
        got = lax.ppermute(piece, "o", [(s, (s + d) % r) for s in range(r)])
        out = lax.dynamic_update_slice(out, got[None], ((o - d) % r, 0, 0))
    return out


def gather_rows(part, p):
    if p != 4:
        return lax.all_gather(part, "i", axis=1)
    i = lax.axis_index("i")
    half = part.shape[0] // 2
    near = lax.ppermute(part, "i", [(s, s ^ 1) for s in range(p)])
    far = lax.ppermute(part, "i", [(s, s ^ 2) for s in range(p)])
    low = lax.ppermute(near[:half], "i", [(s, s ^ 2) for s in range(p)])
    high = lax.ppermute(far[half:], "i", [(s, s ^ 1) for s in range(p)])
    out = jnp.zeros((part.shape[0], p) + part.shape[1:], part.dtype)
    put = lambda out, piece, at, to: lax.dynamic_update_slice(out, piece[:, None], (at, to, 0, 0))
    out = put(out, part, 0, i)
    out = put(out, near, 0, i ^ 1)
    out = put(out, far, 0, i ^ 2)
    out = put(out, low, 0, i ^ 3)
    return put(out, high, half, i ^ 3)


def gather_path(block, r):
    o = lax.axis_index("o")
    up, down = [block], [block]
    for k in range(1, r):
        up.append(lax.ppermute(up[-1], "o", [(s, s + 1) for s in range(k - 1, r - 1)]))
        down.append(lax.ppermute(down[-1], "o", [(s, s - 1) for s in range(1, r - k + 1)]))
    return [block] + [jnp.where(o >= d, up[d], down[r - d]) for d in range(1, r)]


def by_position(by_distance, r):
    o = lax.axis_index("o")
    ahead = [by_distance[-k % r] for k in range(r)]
    return lax.dynamic_slice_in_dim(jnp.stack(ahead + ahead), (r - o) % r, r, axis=0)


def per_device(
    residual_input,
    cotangent,
    lengths,
    norm_gain_vector,
    gate_projection_weight,
    up_projection_weight,
    down_projection_weight,
    up_adapter_first,
    up_adapter_second,
    down_adapter_first,
    down_adapter_second,
    r,
    p,
):
    f32, bf16 = jnp.float32, jnp.bfloat16
    c, o = lax.axis_index("mp"), lax.axis_index("o")
    seq, part = residual_input.shape
    model_width, rank = up_adapter_first.shape
    mp = model_width // part
    hidden = up_adapter_second.shape[1] // r
    clip_limit = clip_coefficient * math.sqrt(2.0 * rank * (model_width + hidden * r * mp))

    wide = residual_input.astype(f32)
    mean = lax.psum(jnp.sum(wide * wide, axis=1, keepdims=True), "mp") / model_width
    gain = lax.dynamic_slice(norm_gain_vector, (c * part,), (part,)).astype(f32)
    normed = (wide * lax.rsqrt(mean + norm_eps) * gain).astype(bf16)
    live = (lax.broadcasted_iota(jnp.int32, (seq, 1), 0) < lengths[0]).astype(f32)
    grad_out = (cotangent.astype(f32) * live).astype(bf16)

    def whole(weight):
        full = gather_rows(exchange_columns(weight, r), p)
        return full.reshape(model_width, hidden)

    gate_weight = whole(gate_projection_weight)
    up_weight = whole(up_projection_weight)
    down_weight = whole(down_projection_weight)
    normed = [lax.all_gather(b, "mp", axis=1, tiled=True) for b in gather_path(normed, r)]
    grad_out = [lax.all_gather(b, "mp", axis=1, tiled=True) for b in gather_path(grad_out, r)]

    up_second = lax.dynamic_slice(up_adapter_second, (0, o * hidden), (rank, hidden))
    down_first = lax.dynamic_slice(down_adapter_first, (o * hidden, 0), (hidden, rank))
    lat_up, lat_down, back_lat, up_lat = [], [], [], []
    grad_down_first, grad_up_second = [], []
    for n, g in zip(normed, grad_out):
        lat = matmul(n, up_adapter_first).astype(bf16)
        act = jax.nn.silu(matmul(n, gate_weight))
        up = matmul(n, up_weight) + adapter_scale * matmul(lat, up_second)
        hid = (act * up).astype(bf16)
        lat_down.append(contract(down_first, hid, 0, 1))
        back = contract(g, down_adapter_second, 1, 1).astype(bf16)
        grad_hidden = matmul(g, down_weight) + adapter_scale * contract(back, down_first, 1, 1)
        grad_up = (grad_hidden * act).astype(bf16)
        grad_down_first.append(adapter_scale * contract(back, hid, 0, 0))
        grad_up_second.append(adapter_scale * contract(lat, grad_up, 0, 0))
        up_lat.append(contract(up_second, grad_up, 1, 1))

    quarter = model_width // r

    def shared(parts):
        total = lax.psum(by_position(parts, r), ("o", "mp")).astype(bf16)
        return [lax.dynamic_index_in_dim(total, (o - d) % r, 0, keepdims=False) for d in range(r)]

    def second(latents, blocks):
        take = lambda b: lax.dynamic_slice(b, (0, o * quarter), (seq, quarter))
        return [adapter_scale * matmul(lt, take(b)) for lt, b in zip(latents, blocks)]

    grad_down_second = second(shared(lat_down), grad_out)
    grad_up_first = second(shared(up_lat), normed)
    four = [
        jnp.concatenate(q, axis=1)
        for q in zip(grad_up_first, grad_up_second, grad_down_first, grad_down_second)
    ]
    owned = [
        jnp.sum(uf * uf) / mp + jnp.sum(ds * ds) / mp + jnp.sum(us * us) + jnp.sum(df * df)
        for uf, us, df, ds in zip(grad_up_first, grad_up_second, grad_down_first, grad_down_second)
    ]
    squares = lax.psum(by_position(owned, r), ("o", "mp"))
    factor = jnp.minimum(1.0, clip_limit / (jnp.sqrt(squares) + 1e-06))
    total = sum(lax.dynamic_index_in_dim(factor, (o - d) % r, 0, keepdims=False) * four[d] for d in range(r))
    sizes = [quarter, hidden, hidden, quarter]
    pieces, start = [], 0
    for size in sizes:
        pieces.append(total[:, start : start + size].reshape(rank, p, size // p))
        start += size
    pieces = jnp.moveaxis(jnp.concatenate(pieces, axis=2), 1, 0)
    mine = jnp.sum(lax.all_to_all(pieces, "i", 0, 0, tiled=True), axis=0)
    outs, start = [], 0
    for size in sizes:
        outs.append(mine[:, start : start + size // p])
        start += size // p
    return outs[0].T, outs[1], outs[2].T, outs[3]


def solution(mesh):
    dp, mp = mesh.shape["dp"], mesh.shape["mp"]
    r = outer_count(dp)
    p = dp // r
    grid = Mesh(mesh.devices.reshape(r, p, mp), ("o", "i", "mp"))
    rows = ("o", "i")

    def body(*args):
        return per_device(*args, r=r, p=p)

    return jax.shard_map(
        body,
        mesh=grid,
        in_specs=(
            P(rows, "mp"),
            P(rows, "mp"),
            P(rows),
            P(),
            P(rows, "mp"),
            P(rows, "mp"),
            P(rows, "mp"),
            P(),
            P(None, "mp"),
            P("mp", None),
            P(),
        ),
        out_specs=(P(rows, None), P(None, ("mp", "o", "i")), P(("mp", "o", "i"), None), P(None, rows)),
        check_vma=False,
    )
```

```python
import math

import jax
import jax.numpy as jnp
from jax import lax
from jax.experimental import pallas as pl
from jax.experimental.pallas import tpu as pltpu
from jax.sharding import Mesh, PartitionSpec as P

norm_eps = 1e-06
adapter_scale = 2.0
clip_coefficient = 0.005


def matmul(left, right):
    return jnp.dot(left, right, preferred_element_type=jnp.float32)


def contract(left, right, left_dim, right_dim):
    return lax.dot_general(
        left, right, (((left_dim,), (right_dim,)), ((), ())), preferred_element_type=jnp.float32
    )


def outer_count(dp):
    return min(r for r in range(1, dp + 1) if dp % r == 0 and r * r >= dp)


def after(value, done):
    return lax.optimization_barrier((value, done))[0]


def copied(shape, places, arrays, plan, into=None):
    count = len(arrays)

    def kernel(place, *refs):
        sources, target, staged = refs[:count], refs[-count - 3], refs[-count - 2 : -2]
        loads = [
            pltpu.make_async_copy(source, stage, refs[-2].at[k])
            for k, (source, stage) in enumerate(zip(sources, staged))
        ]
        stores = [
            pltpu.make_async_copy(stage, to, refs[-1].at[k])
            for k, (stage, to) in enumerate(zip(staged, plan(place, target)))
        ]
        for load in loads:
            load.start()
        for load, store in zip(loads, stores):
            load.wait()
            store.start()
        for store in stores:
            store.wait()

    anywhere = pl.BlockSpec(memory_space=pl.ANY)
    extra = [] if into is None else [into]
    return pl.pallas_call(
        kernel,
        out_shape=jax.ShapeDtypeStruct(shape, arrays[0].dtype),
        in_specs=[pl.BlockSpec(memory_space=pltpu.SMEM)] + [anywhere] * (count + len(extra)),
        out_specs=anywhere,
        scratch_shapes=[pltpu.VMEM(a.shape, a.dtype) for a in arrays]
        + [pltpu.SemaphoreType.DMA((count,)), pltpu.SemaphoreType.DMA((count,))],
        input_output_aliases={} if into is None else {1 + count: 0},
    )(places, *arrays, *extra)


def column_pieces(weight, r):
    o = lax.axis_index("o")
    rows, width = weight.shape[0], weight.shape[1] // r
    return [lax.dynamic_slice(weight, (0, (o + d) % r * width), (rows, width)) for d in range(r)]


def exchange(pieces, r):
    return [pieces[0]] + [
        lax.ppermute(pieces[d], "o", [(s, (s + d) % r) for s in range(r)]) for d in range(1, r)
    ]


def by_position(got, r):
    o = lax.axis_index("o")
    places = (o - jnp.arange(r, dtype=jnp.int32)) % r
    return copied(
        (r,) + got[0].shape,
        places,
        got,
        lambda place, target: [target.at[place[d]] for d in range(r)],
    )


def neighbours(part, p):
    if p != 4:
        return [lax.all_gather(part, "i", axis=1)], []
    half = part.shape[0] // 2
    near = [lax.ppermute(part, "i", [(s, s ^ bit) for s in range(p)]) for bit in (1, 2)]
    return near, [near[0][:half], near[1][half:]]


def assembled(part, near, passed, p):
    if p != 4:
        return near[0].reshape(-1, part.shape[-1])
    half = part.shape[0] // 2
    places = lax.axis_index("i") ^ jnp.arange(p, dtype=jnp.int32)
    shape = (part.shape[0], p) + part.shape[1:]
    corner = [
        lax.ppermute(piece, "i", [(s, s ^ bit) for s in range(p)]) for piece, bit in zip(passed, (2, 1))
    ]
    out = copied(
        shape,
        places,
        [part] + near,
        lambda place, target: [target.at[:, place[k]] for k in range(3)],
    )
    out = copied(
        shape,
        places,
        corner,
        lambda place, target: [target.at[:half, place[3]], target.at[half:, place[3]]],
        out,
    )
    return out.reshape(-1, part.shape[-1])


def arrival(at, n, r):
    sides = list(range(at + 1, r)), list(range(at - 1, -1, -1))
    first, second = sides if at < r // 2 else sides[::-1]
    return ([at] + first + second)[n]


def gather_path(half, r):
    o = lax.axis_index("o")
    up, down = [half], [half]
    for k in range(1, r):
        up.append(lax.ppermute(up[-1], "o", [(s, s + 1) for s in range(k - 1, r - 1)]))
        down.append(lax.ppermute(down[-1], "o", [(s, s - 1) for s in range(1, r - k + 1)]))
    blocks = [half]
    for n in range(1, r):
        values = []
        for at in range(r):
            source = arrival(at, n, r)
            values.append(up[at - source] if source < at else down[source - at])
        distinct = list({id(v): v for v in values}.values())
        fenced = dict(zip(map(id, distinct), lax.optimization_barrier(distinct)))
        block = fenced[id(values[0])]
        for at in range(1, r):
            if values[at] is not values[at - 1]:
                block = jnp.where(o >= at, fenced[id(values[at])], block)
        blocks.append(block)
    return blocks, (up[1], down[1])


def across(block, mp):
    width = block.shape[1] // 2
    if mp != 2:
        both = lax.all_gather(block, "mp", axis=0)
        whole = lambda a: a.swapaxes(0, 1).reshape(block.shape[0], -1)
        return whole(both[:, :, :width]), whole(both[:, :, width:])
    other = lax.ppermute(block, "mp", [(0, 1), (1, 0)])
    first = lax.axis_index("mp") == 0
    south, north = jnp.where(first, block, other), jnp.where(first, other, block)
    return (
        jnp.concatenate([south[:, :width], north[:, :width]], axis=1),
        jnp.concatenate([south[:, width:], north[:, width:]], axis=1),
    )


def per_device(
    residual_input,
    cotangent,
    lengths,
    norm_gain_vector,
    gate_projection_weight,
    up_projection_weight,
    down_projection_weight,
    up_adapter_first,
    up_adapter_second,
    down_adapter_first,
    down_adapter_second,
    r,
    p,
):
    f32, bf16 = jnp.float32, jnp.bfloat16
    c, o = lax.axis_index("mp"), lax.axis_index("o")
    seq, part = residual_input.shape
    model_width, rank = up_adapter_first.shape
    mp = model_width // part
    block = model_width // (r * p)
    hidden = up_adapter_second.shape[1] // r
    clip_limit = clip_coefficient * math.sqrt(2.0 * rank * (model_width + hidden * r * mp))

    gate_cut = column_pieces(gate_projection_weight, r)
    up_cut = column_pieces(up_projection_weight, r)
    down_cut = column_pieces(down_projection_weight, r)

    wide = after(residual_input, gate_cut).astype(f32)
    mean = lax.psum(jnp.sum(wide * wide, axis=1, keepdims=True), "mp") / model_width
    gain = lax.dynamic_slice(norm_gain_vector, (c * part,), (part,)).astype(f32)
    normed = (wide * lax.rsqrt(mean + norm_eps) * gain).astype(bf16)
    live = (lax.broadcasted_iota(jnp.int32, (seq, 1), 0) < lengths[0]).astype(f32)
    grad_out = (cotangent.astype(f32) * live).astype(bf16)

    tokens, first_tokens = gather_path(jnp.concatenate([normed, grad_out], axis=1), r)
    gate_part = by_position(exchange(gate_cut, r), r)
    gate_near, gate_pass = neighbours(gate_part, p)
    up_part = by_position(exchange(up_cut, r), r)
    up_near, up_pass = neighbours(up_part, p)
    down_got = exchange(down_cut, r)
    down_part = by_position(after(down_got, (gate_pass, up_pass, first_tokens)), r)
    down_near, down_pass = neighbours(down_part, p)
    gate_weight = assembled(gate_part, gate_near, gate_pass, p)
    up_weight = assembled(up_part, up_near, up_pass, p)
    down_weight = assembled(down_part, down_near, down_pass, p)
    normed, grad_out = zip(*[across(t, mp) for t in tokens])
    table = jnp.array([[arrival(at, n, r) for n in range(r)] for at in range(r)], jnp.int32)
    places = lax.dynamic_index_in_dim(table, o, 0, keepdims=False)

    up_second = lax.dynamic_slice(up_adapter_second, (0, o * hidden), (rank, hidden))
    down_first = lax.dynamic_slice(down_adapter_first, (o * hidden, 0), (hidden, rank))

    def square(array):
        return jnp.sum(array * array)

    def cut(array, k, group, axis):
        at = group.index(k) * seq
        return lax.slice_in_dim(array, at, at + seq, axis=axis)

    lat, act, hid = {}, {}, {}
    for group in [[k] for k in range(r)]:
        n = jnp.concatenate([normed[k] for k in group], axis=0)
        group_lat = contract(up_adapter_first, n, 0, 1).astype(bf16)
        group_act = jax.nn.silu(matmul(n, gate_weight))
        up = matmul(n, up_weight) + adapter_scale * contract(group_lat, up_second, 0, 0)
        group_hid = (group_act * up).astype(bf16)
        for k in group:
            lat[k] = cut(group_lat, k, group, 1)
            act[k] = cut(group_act, k, group, 0)
            hid[k] = cut(group_hid, k, group, 0)

    sums = jnp.zeros((2 * rank + 2, r * seq), bf16)
    grad_up_second, grad_down_first = [], []
    for group in [[k] for k in range(r)]:
        g = jnp.concatenate([grad_out[k] for k in group], axis=0)
        back = contract(down_adapter_second, g, 1, 1).astype(bf16)
        grad_hidden = matmul(g, down_weight) + adapter_scale * contract(back, down_first, 0, 1)
        grad_up = jnp.concatenate([act[k] for k in group], axis=0) * grad_hidden
        grad_up = grad_up.astype(bf16)
        up_lat = contract(up_second, grad_up, 1, 1)
        for k in group:
            grad_down_first.append(adapter_scale * matmul(cut(back, k, group, 1), hid[k]))
            grad_up_second.append(adapter_scale * matmul(lat[k], cut(grad_up, k, group, 0)))
            split = square(grad_down_first[k]) + square(grad_up_second[k])
            high = split.astype(bf16)
            low = (split - high.astype(f32)).astype(bf16)
            partial = [
                contract(down_first, hid[k], 0, 1).astype(bf16),
                cut(up_lat, k, group, 1).astype(bf16),
                jnp.broadcast_to(high, (1, seq)),
                jnp.broadcast_to(low, (1, seq)),
            ]
            partial = jnp.concatenate(partial, axis=0)
            sums = lax.dynamic_update_slice(sums, partial, (0, places[k] * seq))

    products = []
    for tokens in (grad_out, normed):
        for t in tokens:
            products.append(contract(t, t, 1, 1))
    products = jnp.stack(lax.optimization_barrier(products))
    share = lambda t: lax.dynamic_slice(t, (0, o * p * block), (seq, p * block))
    grad_share = jnp.concatenate([share(g) for g in grad_out], axis=0)
    normed_share = jnp.concatenate([share(n) for n in normed], axis=0)

    sums = jnp.sum(lax.all_gather(sums, ("o", "mp"), axis=0).astype(f32), axis=0)
    sums = jnp.concatenate(
        [lax.dynamic_slice(sums, (0, places[k] * seq), (2 * rank + 2, seq)) for k in range(r)], axis=1
    )
    lat_down = sums[:rank].astype(bf16).astype(f32)
    up_lat = sums[rank : 2 * rank].astype(bf16).astype(f32)
    latents = jnp.concatenate([lat_down, up_lat], axis=1).reshape(rank, 2 * r, seq).swapaxes(0, 1)
    through = lax.dot_general(
        latents, products, (((2,), (1,)), ((0,), (0,))), precision=lax.Precision.HIGHEST
    )
    squares = adapter_scale**2 * jnp.sum(latents * through, axis=(1, 2)).reshape(2, r).sum(axis=0)
    squares = squares + sums[2 * rank, ::seq] + sums[2 * rank + 1, ::seq]
    factors = jnp.minimum(1.0, clip_limit / (jnp.sqrt(squares) + 1e-06))

    def clipped(arrays):
        return sum(factors[k] * array for k, array in enumerate(arrays))

    by_token = jnp.repeat(adapter_scale * factors, seq)[None]

    def token_gradient(latent, tokens):
        scaled = by_token * latent
        high = scaled.astype(bf16)
        low = (scaled - high.astype(f32)).astype(bf16)
        both = matmul(jnp.concatenate([high, low], axis=0), tokens)
        return both[:rank] + both[rank:]

    sizes = (block, hidden // p, hidden // p, block)
    pieces = (
        token_gradient(up_lat, normed_share),
        clipped(grad_up_second),
        clipped(grad_down_first),
        token_gradient(lat_down, grad_share),
    )
    pieces = [a.reshape(rank, p, size).swapaxes(0, 1) for a, size in zip(pieces, sizes)]
    pieces = jnp.concatenate(pieces, axis=2).astype(bf16)
    total = lax.all_to_all(pieces, "i", 0, 0, tiled=True)
    total = jnp.sum(total.reshape(p, rank, -1).astype(f32), axis=0)
    outs, start = [], 0
    for size in sizes:
        outs.append(total[:, start : start + size])
        start += size
    return outs[0].T, outs[1], outs[2].T, outs[3]


def solution(mesh):
    dp, mp = mesh.shape["dp"], mesh.shape["mp"]
    r = outer_count(dp)
    p = dp // r
    grid = Mesh(mesh.devices.reshape(r, p, mp), ("o", "i", "mp"))
    rows = ("o", "i")

    def body(*args):
        return per_device(*args, r=r, p=p)

    return jax.shard_map(
        body,
        mesh=grid,
        in_specs=(
            P(rows, "mp"),
            P(rows, "mp"),
            P(rows),
            P(),
            P(rows, "mp"),
            P(rows, "mp"),
            P(rows, "mp"),
            P(),
            P(None, "mp"),
            P("mp", None),
            P(),
        ),
        out_specs=(P(rows, None), P(None, ("mp", "o", "i")), P(("mp", "o", "i"), None), P(None, rows)),
        check_vma=False,
    )
```

```python
import math

import jax
import jax.numpy as jnp
from jax import lax
from jax.experimental import pallas as pl
from jax.experimental.pallas import tpu as pltpu
from jax.sharding import Mesh, PartitionSpec as P

norm_eps = 1e-06
adapter_scale = 2.0
clip_coefficient = 0.005


def matmul(left, right):
    return jnp.dot(left, right, preferred_element_type=jnp.float32)


def contract(left, right, left_dim, right_dim):
    return lax.dot_general(
        left, right, (((left_dim,), (right_dim,)), ((), ())), preferred_element_type=jnp.float32
    )


def outer_count(dp):
    return min(r for r in range(1, dp + 1) if dp % r == 0 and r * r >= dp)


def after(value, done):
    return lax.optimization_barrier((value, done))[0]


def copied(shape, places, arrays, plan, into=None):
    count = len(arrays)

    def kernel(place, *refs):
        sources, target, staged = refs[:count], refs[-count - 3], refs[-count - 2 : -2]
        loads = [
            pltpu.make_async_copy(source, stage, refs[-2].at[k])
            for k, (source, stage) in enumerate(zip(sources, staged))
        ]
        stores = [
            pltpu.make_async_copy(stage, to, refs[-1].at[k])
            for k, (stage, to) in enumerate(zip(staged, plan(place, target)))
        ]
        for load in loads:
            load.start()
        for load, store in zip(loads, stores):
            load.wait()
            store.start()
        for store in stores:
            store.wait()

    anywhere = pl.BlockSpec(memory_space=pl.ANY)
    extra = [] if into is None else [into]
    return pl.pallas_call(
        kernel,
        out_shape=jax.ShapeDtypeStruct(shape, arrays[0].dtype),
        in_specs=[pl.BlockSpec(memory_space=pltpu.SMEM)] + [anywhere] * (count + len(extra)),
        out_specs=anywhere,
        scratch_shapes=[pltpu.VMEM(a.shape, a.dtype) for a in arrays]
        + [pltpu.SemaphoreType.DMA((count,)), pltpu.SemaphoreType.DMA((count,))],
        input_output_aliases={} if into is None else {1 + count: 0},
        compiler_params=pltpu.CompilerParams(
            vmem_limit_bytes=(1 << 20) + 2 * sum(a.size * a.dtype.itemsize for a in arrays)
        ),
    )(places, *arrays, *extra)


def gathered(shape, places, arrays, plan, into=None):
    count = len(arrays)

    def kernel(place, *refs):
        copies = [
            pltpu.make_async_copy(source, to, refs[-1].at[k])
            for k, (source, to) in enumerate(zip(refs[:count], plan(place, refs[-2])))
        ]
        for copy in copies:
            copy.start()
        for copy in copies:
            copy.wait()

    anywhere, on_chip = pl.BlockSpec(memory_space=pl.ANY), pl.BlockSpec(memory_space=pltpu.VMEM)
    extra = [] if into is None else [into]
    return pl.pallas_call(
        kernel,
        out_shape=pltpu.VMEM(shape, arrays[0].dtype),
        in_specs=[pl.BlockSpec(memory_space=pltpu.SMEM)] + [anywhere] * count + [on_chip] * len(extra),
        out_specs=on_chip,
        scratch_shapes=[pltpu.SemaphoreType.DMA((count,))],
        input_output_aliases={} if into is None else {1 + count: 0},
        compiler_params=pltpu.CompilerParams(vmem_limit_bytes=1 << 20),
    )(places, *arrays, *extra)


def column_pieces(weight, r):
    o = lax.axis_index("o")
    rows, width = weight.shape[0], weight.shape[1] // r
    return [lax.dynamic_slice(weight, (0, (o + d) % r * width), (rows, width)) for d in range(r)]


def exchange(pieces, r):
    return [pieces[0]] + [
        lax.ppermute(pieces[d], "o", [(s, (s + d) % r) for s in range(r)]) for d in range(1, r)
    ]


def by_position(got, r):
    o = lax.axis_index("o")
    places = (o - jnp.arange(r, dtype=jnp.int32)) % r
    return copied(
        (r,) + got[0].shape,
        places,
        got,
        lambda place, target: [target.at[place[d]] for d in range(r)],
    )


def neighbours(part, p):
    if p != 4:
        return [lax.all_gather(part, "i", axis=1)], []
    half = part.shape[0] // 2
    near = [lax.ppermute(part, "i", [(s, s ^ bit) for s in range(p)]) for bit in (1, 2)]
    return near, [near[0][:half], near[1][half:]]


def assembled(part, near, passed, p):
    if p != 4:
        return near[0].reshape(-1, part.shape[-1])
    half = part.shape[0] // 2
    places = lax.axis_index("i") ^ jnp.arange(p, dtype=jnp.int32)
    shape = (part.shape[0], p) + part.shape[1:]
    corner = [
        lax.ppermute(piece, "i", [(s, s ^ bit) for s in range(p)]) for piece, bit in zip(passed, (2, 1))
    ]
    out = gathered(
        shape,
        places,
        [part] + near,
        lambda place, target: [target.at[:, place[k]] for k in range(3)],
    )
    out = gathered(
        shape,
        places,
        corner,
        lambda place, target: [target.at[:half, place[3]], target.at[half:, place[3]]],
        out,
    )
    return out.reshape(-1, part.shape[-1])


def arrival(at, n, r):
    sides = list(range(at + 1, r)), list(range(at - 1, -1, -1))
    first, second = sides if at < r // 2 else sides[::-1]
    return ([at] + first + second)[n]


def gather_path(half, r):
    o = lax.axis_index("o")
    up, down = [half], [half]
    for k in range(1, r):
        up.append(lax.ppermute(up[-1], "o", [(s, s + 1) for s in range(k - 1, r - 1)]))
        down.append(lax.ppermute(down[-1], "o", [(s, s - 1) for s in range(1, r - k + 1)]))
    blocks = [half]
    for n in range(1, r):
        values = []
        for at in range(r):
            source = arrival(at, n, r)
            values.append(up[at - source] if source < at else down[source - at])
        distinct = list({id(v): v for v in values}.values())
        fenced = dict(zip(map(id, distinct), lax.optimization_barrier(distinct)))
        block = fenced[id(values[0])]
        for at in range(1, r):
            if values[at] is not values[at - 1]:
                block = jnp.where(o >= at, fenced[id(values[at])], block)
        blocks.append(block)
    return blocks, (up[1], down[1])


def across(block, mp):
    width = block.shape[1] // 2
    if mp != 2:
        both = lax.all_gather(block, "mp", axis=0)
        whole = lambda a: a.swapaxes(0, 1).reshape(block.shape[0], -1)
        return whole(both[:, :, :width]), whole(both[:, :, width:])
    other = lax.ppermute(block, "mp", [(0, 1), (1, 0)])
    c = lax.axis_index("mp")

    def kernel(place, own, received, normed, gradient, sems):
        copies = []
        for k, (source, at) in enumerate(((own, place[0]), (received, place[1]))):
            columns = pl.ds(pl.multiple_of(at * width, 128), width)
            for j, target in enumerate((normed, gradient)):
                part = source.at[:, j * width : (j + 1) * width]
                copies.append(pltpu.make_async_copy(part, target.at[:, columns], sems.at[2 * k + j]))
        for copy in copies:
            copy.start()
        for copy in copies:
            copy.wait()

    anywhere, on_chip = pl.BlockSpec(memory_space=pl.ANY), pl.BlockSpec(memory_space=pltpu.VMEM)
    shape = (block.shape[0], 2 * width)
    return pl.pallas_call(
        kernel,
        out_shape=[pltpu.VMEM(shape, block.dtype)] * 2,
        in_specs=[pl.BlockSpec(memory_space=pltpu.SMEM), anywhere, anywhere],
        out_specs=[on_chip] * 2,
        scratch_shapes=[pltpu.SemaphoreType.DMA((4,))],
        compiler_params=pltpu.CompilerParams(vmem_limit_bytes=1 << 20),
    )(jnp.stack([c, 1 - c]).astype(jnp.int32), block, other)


def per_device(
    residual_input,
    cotangent,
    lengths,
    norm_gain_vector,
    gate_projection_weight,
    up_projection_weight,
    down_projection_weight,
    up_adapter_first,
    up_adapter_second,
    down_adapter_first,
    down_adapter_second,
    r,
    p,
):
    f32, bf16 = jnp.float32, jnp.bfloat16
    c, o = lax.axis_index("mp"), lax.axis_index("o")
    seq, part = residual_input.shape
    model_width, rank = up_adapter_first.shape
    mp = model_width // part
    block = model_width // (r * p)
    hidden = up_adapter_second.shape[1] // r
    clip_limit = clip_coefficient * math.sqrt(2.0 * rank * (model_width + hidden * r * mp))

    gate_cut = column_pieces(gate_projection_weight, r)
    up_cut = column_pieces(up_projection_weight, r)
    down_cut = column_pieces(down_projection_weight, r)

    wide = after(residual_input, gate_cut).astype(f32)
    mean = lax.psum(jnp.sum(wide * wide, axis=1, keepdims=True), "mp") / model_width
    gain = lax.dynamic_slice(norm_gain_vector, (c * part,), (part,)).astype(f32)
    normed = (wide * lax.rsqrt(mean + norm_eps) * gain).astype(bf16)
    live = (lax.broadcasted_iota(jnp.int32, (seq, 1), 0) < lengths[0]).astype(f32)
    grad_out = (cotangent.astype(f32) * live).astype(bf16)

    tokens, first_tokens = gather_path(jnp.concatenate([normed, grad_out], axis=1), r)
    gate_part = by_position(exchange(gate_cut, r), r)
    gate_near, gate_pass = neighbours(gate_part, p)
    up_part = by_position(exchange(up_cut, r), r)
    up_near, up_pass = neighbours(up_part, p)
    down_got = exchange(down_cut, r)
    down_part = by_position(after(down_got, (gate_pass, up_pass, first_tokens)), r)
    down_near, down_pass = neighbours(down_part, p)
    gate_weight = assembled(gate_part, gate_near, gate_pass, p)
    up_weight = assembled(up_part, up_near, up_pass, p)
    down_weight = assembled(down_part, down_near, down_pass, p)
    normed, grad_out = zip(*[across(t, mp) for t in tokens])
    table = jnp.array([[arrival(at, n, r) for n in range(r)] for at in range(r)], jnp.int32)
    places = lax.dynamic_index_in_dim(table, o, 0, keepdims=False)

    up_second = lax.dynamic_slice(up_adapter_second, (0, o * hidden), (rank, hidden))
    down_first = lax.dynamic_slice(down_adapter_first, (o * hidden, 0), (hidden, rank))

    def square(array):
        return jnp.sum(array * array)

    def cut(array, k, group, axis):
        at = group.index(k) * seq
        return lax.slice_in_dim(array, at, at + seq, axis=axis)

    lat, act, hid = {}, {}, {}
    for group in [[k] for k in range(r)]:
        n = jnp.concatenate([normed[k] for k in group], axis=0)
        group_lat = contract(up_adapter_first, n, 0, 1).astype(bf16)
        group_act = jax.nn.silu(matmul(n, gate_weight))
        up = matmul(n, up_weight) + adapter_scale * contract(group_lat, up_second, 0, 0)
        group_hid = (group_act * up).astype(bf16)
        for k in group:
            lat[k] = cut(group_lat, k, group, 1)
            act[k] = cut(group_act, k, group, 0)
            hid[k] = cut(group_hid, k, group, 0)

    sums = jnp.zeros((2 * rank + 2, r * seq), bf16)
    grad_up_second, grad_down_first = [], []
    for group in [[k] for k in range(r)]:
        g = jnp.concatenate([grad_out[k] for k in group], axis=0)
        back = contract(down_adapter_second, g, 1, 1).astype(bf16)
        grad_hidden = matmul(g, down_weight) + adapter_scale * contract(back, down_first, 0, 1)
        grad_up = jnp.concatenate([act[k] for k in group], axis=0) * grad_hidden
        grad_up = grad_up.astype(bf16)
        up_lat = contract(up_second, grad_up, 1, 1)
        for k in group:
            grad_down_first.append(adapter_scale * matmul(cut(back, k, group, 1), hid[k]))
            grad_up_second.append(adapter_scale * matmul(lat[k], cut(grad_up, k, group, 0)))
            split = square(grad_down_first[k]) + square(grad_up_second[k])
            high = split.astype(bf16)
            low = (split - high.astype(f32)).astype(bf16)
            partial = [
                contract(down_first, hid[k], 0, 1).astype(bf16),
                cut(up_lat, k, group, 1).astype(bf16),
                jnp.broadcast_to(high, (1, seq)),
                jnp.broadcast_to(low, (1, seq)),
            ]
            partial = jnp.concatenate(partial, axis=0)
            sums = lax.dynamic_update_slice(sums, partial, (0, places[k] * seq))

    products = []
    for tokens in (grad_out, normed):
        for t in tokens:
            products.append(contract(t, t, 1, 1))
    products = jnp.stack(lax.optimization_barrier(products))
    share = lambda t: lax.dynamic_slice(t, (0, o * p * block), (seq, p * block))
    grad_share = jnp.concatenate([share(g) for g in grad_out], axis=0)
    normed_share = jnp.concatenate([share(n) for n in normed], axis=0)

    sums = jnp.sum(lax.all_gather(sums, ("o", "mp"), axis=0).astype(f32), axis=0)
    sums = jnp.concatenate(
        [lax.dynamic_slice(sums, (0, places[k] * seq), (2 * rank + 2, seq)) for k in range(r)], axis=1
    )
    lat_down = sums[:rank].astype(bf16).astype(f32)
    up_lat = sums[rank : 2 * rank].astype(bf16).astype(f32)
    latents = jnp.concatenate([lat_down, up_lat], axis=1).reshape(rank, 2 * r, seq).swapaxes(0, 1)
    through = lax.dot_general(
        latents, products, (((2,), (1,)), ((0,), (0,))), precision=lax.Precision.HIGHEST
    )
    squares = adapter_scale**2 * jnp.sum(latents * through, axis=(1, 2)).reshape(2, r).sum(axis=0)
    squares = squares + sums[2 * rank, ::seq] + sums[2 * rank + 1, ::seq]
    factors = jnp.minimum(1.0, clip_limit / (jnp.sqrt(squares) + 1e-06))

    def clipped(arrays):
        return sum(factors[k] * array for k, array in enumerate(arrays))

    by_token = jnp.repeat(adapter_scale * factors, seq)[None]

    def token_gradient(latent, tokens):
        scaled = by_token * latent
        high = scaled.astype(bf16)
        low = (scaled - high.astype(f32)).astype(bf16)
        both = matmul(jnp.concatenate([high, low], axis=0), tokens)
        return both[:rank] + both[rank:]

    sizes = (block, hidden // p, hidden // p, block)
    pieces = (
        token_gradient(up_lat, normed_share),
        clipped(grad_up_second),
        clipped(grad_down_first),
        token_gradient(lat_down, grad_share),
    )
    pieces = [a.reshape(rank, p, size).swapaxes(0, 1) for a, size in zip(pieces, sizes)]
    pieces = jnp.concatenate(pieces, axis=2).astype(bf16)
    total = lax.all_to_all(pieces, "i", 0, 0, tiled=True)
    total = jnp.sum(total.reshape(p, rank, -1).astype(f32), axis=0)
    outs, start = [], 0
    for size in sizes:
        outs.append(total[:, start : start + size])
        start += size
    return outs[0].T, outs[1], outs[2].T, outs[3]


def solution(mesh):
    dp, mp = mesh.shape["dp"], mesh.shape["mp"]
    r = outer_count(dp)
    p = dp // r
    grid = Mesh(mesh.devices.reshape(r, p, mp), ("o", "i", "mp"))
    rows = ("o", "i")

    def body(*args):
        return per_device(*args, r=r, p=p)

    return jax.shard_map(
        body,
        mesh=grid,
        in_specs=(
            P(rows, "mp"),
            P(rows, "mp"),
            P(rows),
            P(),
            P(rows, "mp"),
            P(rows, "mp"),
            P(rows, "mp"),
            P(),
            P(None, "mp"),
            P("mp", None),
            P(),
        ),
        out_specs=(P(rows, None), P(None, ("mp", "o", "i")), P(("mp", "o", "i"), None), P(None, rows)),
        check_vma=False,
    )
```

```python
import math

import jax
import jax.numpy as jnp
from jax import lax
from jax.experimental import pallas as pl
from jax.experimental.pallas import tpu as pltpu
from jax.sharding import Mesh, PartitionSpec as P

norm_eps = 1e-06
adapter_scale = 2.0
clip_coefficient = 0.005


def matmul(left, right):
    return jnp.dot(left, right, preferred_element_type=jnp.float32)


def contract(left, right, left_dim, right_dim):
    return lax.dot_general(
        left, right, (((left_dim,), (right_dim,)), ((), ())), preferred_element_type=jnp.float32
    )


def outer_count(dp):
    return min(r for r in range(1, dp + 1) if dp % r == 0 and r * r >= dp)


def after(value, done):
    return lax.optimization_barrier((value, done))[0]


def copied(shape, places, arrays, plan, into=None):
    count = len(arrays)

    def kernel(place, *refs):
        sources, target, staged = refs[:count], refs[-count - 3], refs[-count - 2 : -2]
        loads = [
            pltpu.make_async_copy(source, stage, refs[-2].at[k])
            for k, (source, stage) in enumerate(zip(sources, staged))
        ]
        stores = [
            pltpu.make_async_copy(stage, to, refs[-1].at[k])
            for k, (stage, to) in enumerate(zip(staged, plan(place, target)))
        ]
        for load in loads:
            load.start()
        for load, store in zip(loads, stores):
            load.wait()
            store.start()
        for store in stores:
            store.wait()

    anywhere = pl.BlockSpec(memory_space=pl.ANY)
    extra = [] if into is None else [into]
    return pl.pallas_call(
        kernel,
        out_shape=jax.ShapeDtypeStruct(shape, arrays[0].dtype),
        in_specs=[pl.BlockSpec(memory_space=pltpu.SMEM)] + [anywhere] * (count + len(extra)),
        out_specs=anywhere,
        scratch_shapes=[pltpu.VMEM(a.shape, a.dtype) for a in arrays]
        + [pltpu.SemaphoreType.DMA((count,)), pltpu.SemaphoreType.DMA((count,))],
        input_output_aliases={} if into is None else {1 + count: 0},
        compiler_params=pltpu.CompilerParams(
            vmem_limit_bytes=(1 << 20) + 2 * sum(a.size * a.dtype.itemsize for a in arrays)
        ),
    )(places, *arrays, *extra)


def gathered(shape, places, arrays, plan, into=None):
    count = len(arrays)

    def kernel(place, *refs):
        copies = [
            pltpu.make_async_copy(source, to, refs[-1].at[k])
            for k, (source, to) in enumerate(zip(refs[:count], plan(place, refs[-2])))
        ]
        for copy in copies:
            copy.start()
        for copy in copies:
            copy.wait()

    anywhere, on_chip = pl.BlockSpec(memory_space=pl.ANY), pl.BlockSpec(memory_space=pltpu.VMEM)
    extra = [] if into is None else [into]
    return pl.pallas_call(
        kernel,
        out_shape=pltpu.VMEM(shape, arrays[0].dtype),
        in_specs=[pl.BlockSpec(memory_space=pltpu.SMEM)] + [anywhere] * count + [on_chip] * len(extra),
        out_specs=on_chip,
        scratch_shapes=[pltpu.SemaphoreType.DMA((count,))],
        input_output_aliases={} if into is None else {1 + count: 0},
        compiler_params=pltpu.CompilerParams(vmem_limit_bytes=1 << 20),
    )(places, *arrays, *extra)


def column_pieces(weight, r):
    o = lax.axis_index("o")
    rows, width = weight.shape[0], weight.shape[1] // r
    return [lax.dynamic_slice(weight, (0, (o + d) % r * width), (rows, width)) for d in range(r)]


def exchange(pieces, r):
    return [pieces[0]] + [
        lax.ppermute(pieces[d], "o", [(s, (s + d) % r) for s in range(r)]) for d in range(1, r)
    ]


def by_position(got, r):
    o = lax.axis_index("o")
    places = (o - jnp.arange(r, dtype=jnp.int32)) % r
    return copied(
        (r,) + got[0].shape,
        places,
        got,
        lambda place, target: [target.at[place[d]] for d in range(r)],
    )


def neighbours(part, p):
    if p != 4:
        return [lax.all_gather(part, "i", axis=1)], []
    half = part.shape[0] // 2
    near = [lax.ppermute(part, "i", [(s, s ^ bit) for s in range(p)]) for bit in (1, 2)]
    return near, [near[0][:half], near[1][half:]]


def assembled(part, near, passed, p):
    if p != 4:
        return near[0].reshape(-1, part.shape[-1])
    half = part.shape[0] // 2
    places = lax.axis_index("i") ^ jnp.arange(p, dtype=jnp.int32)
    shape = (part.shape[0], p) + part.shape[1:]
    corner = [
        lax.ppermute(piece, "i", [(s, s ^ bit) for s in range(p)]) for piece, bit in zip(passed, (2, 1))
    ]
    out = gathered(
        shape,
        places,
        [part] + near,
        lambda place, target: [target.at[:, place[k]] for k in range(3)],
    )
    out = gathered(
        shape,
        places,
        corner,
        lambda place, target: [target.at[:half, place[3]], target.at[half:, place[3]]],
        out,
    )
    return out.reshape(-1, part.shape[-1])


def arrival(at, n, r):
    sides = list(range(at + 1, r)), list(range(at - 1, -1, -1))
    first, second = sides if at < r // 2 else sides[::-1]
    return ([at] + first + second)[n]


def gather_path(half, r):
    o = lax.axis_index("o")
    up, down = [half], [half]
    for k in range(1, r):
        up.append(lax.ppermute(up[-1], "o", [(s, s + 1) for s in range(k - 1, r - 1)]))
        down.append(lax.ppermute(down[-1], "o", [(s, s - 1) for s in range(1, r - k + 1)]))
    blocks = [half]
    for n in range(1, r):
        values = []
        for at in range(r):
            source = arrival(at, n, r)
            values.append(up[at - source] if source < at else down[source - at])
        distinct = list({id(v): v for v in values}.values())
        fenced = dict(zip(map(id, distinct), lax.optimization_barrier(distinct)))
        block = fenced[id(values[0])]
        for at in range(1, r):
            if values[at] is not values[at - 1]:
                block = jnp.where(o >= at, fenced[id(values[at])], block)
        blocks.append(block)
    return blocks, (up[1], down[1])


def across(block, mp):
    width = block.shape[1] // 2
    if mp != 2:
        both = lax.all_gather(block, "mp", axis=0)
        whole = lambda a: a.swapaxes(0, 1).reshape(block.shape[0], -1)
        return whole(both[:, :, :width]), whole(both[:, :, width:])
    other = lax.ppermute(block, "mp", [(0, 1), (1, 0)])
    c = lax.axis_index("mp")

    def kernel(place, own, received, normed, gradient, sems):
        copies = []
        for k, (source, at) in enumerate(((own, place[0]), (received, place[1]))):
            columns = pl.ds(pl.multiple_of(at * width, 128), width)
            for j, target in enumerate((normed, gradient)):
                part = source.at[:, j * width : (j + 1) * width]
                copies.append(pltpu.make_async_copy(part, target.at[:, columns], sems.at[2 * k + j]))
        for copy in copies:
            copy.start()
        for copy in copies:
            copy.wait()

    anywhere, on_chip = pl.BlockSpec(memory_space=pl.ANY), pl.BlockSpec(memory_space=pltpu.VMEM)
    shape = (block.shape[0], 2 * width)
    return pl.pallas_call(
        kernel,
        out_shape=[pltpu.VMEM(shape, block.dtype)] * 2,
        in_specs=[pl.BlockSpec(memory_space=pltpu.SMEM), anywhere, anywhere],
        out_specs=[on_chip] * 2,
        scratch_shapes=[pltpu.SemaphoreType.DMA((4,))],
        compiler_params=pltpu.CompilerParams(vmem_limit_bytes=1 << 20),
    )(jnp.stack([c, 1 - c]).astype(jnp.int32), block, other)


def per_device(
    residual_input,
    cotangent,
    lengths,
    norm_gain_vector,
    gate_projection_weight,
    up_projection_weight,
    down_projection_weight,
    up_adapter_first,
    up_adapter_second,
    down_adapter_first,
    down_adapter_second,
    r,
    p,
):
    f32, bf16 = jnp.float32, jnp.bfloat16
    c, o = lax.axis_index("mp"), lax.axis_index("o")
    seq, part = residual_input.shape
    model_width, rank = up_adapter_first.shape
    mp = model_width // part
    block = model_width // (r * p)
    hidden = up_adapter_second.shape[1] // r
    clip_limit = clip_coefficient * math.sqrt(2.0 * rank * (model_width + hidden * r * mp))

    gate_cut = column_pieces(gate_projection_weight, r)
    up_cut = column_pieces(up_projection_weight, r)
    down_cut = column_pieces(down_projection_weight, r)

    wide = after(residual_input, gate_cut).astype(f32)
    mean = lax.psum(jnp.sum(wide * wide, axis=1, keepdims=True), "mp") / model_width
    gain = lax.dynamic_slice(norm_gain_vector, (c * part,), (part,)).astype(f32)
    normed = (wide * lax.rsqrt(mean + norm_eps) * gain).astype(bf16)
    live = (lax.broadcasted_iota(jnp.int32, (seq, 1), 0) < lengths[0]).astype(f32)
    grad_out = (cotangent.astype(f32) * live).astype(bf16)

    tokens, first_tokens = gather_path(jnp.concatenate([normed, grad_out], axis=1), r)
    gate_part = by_position(exchange(gate_cut, r), r)
    gate_near, gate_pass = neighbours(gate_part, p)
    up_part = by_position(exchange(up_cut, r), r)
    up_near, up_pass = neighbours(up_part, p)
    down_got = exchange(down_cut, r)
    down_part = by_position(after(down_got, (gate_pass, up_pass, first_tokens)), r)
    down_near, down_pass = neighbours(down_part, p)
    gate_weight = assembled(gate_part, gate_near, gate_pass, p)
    up_weight = assembled(up_part, up_near, up_pass, p)
    down_weight = assembled(down_part, down_near, down_pass, p)
    normed, grad_out = zip(*[across(t, mp) for t in tokens])
    table = jnp.array([[arrival(at, n, r) for n in range(r)] for at in range(r)], jnp.int32)
    places = lax.dynamic_index_in_dim(table, o, 0, keepdims=False)

    up_second = lax.dynamic_slice(up_adapter_second, (0, o * hidden), (rank, hidden))
    down_first = lax.dynamic_slice(down_adapter_first, (o * hidden, 0), (hidden, rank))

    def square(array):
        return jnp.sum(array * array)

    def cut(array, k, group, axis):
        at = group.index(k) * seq
        return lax.slice_in_dim(array, at, at + seq, axis=axis)

    lat, act, hid = {}, {}, {}
    for group in [[k] for k in range(r)]:
        n = jnp.concatenate([normed[k] for k in group], axis=0)
        group_lat = contract(up_adapter_first, n, 0, 1).astype(bf16)
        group_act = jax.nn.silu(matmul(n, gate_weight))
        up = matmul(n, up_weight) + adapter_scale * contract(group_lat, up_second, 0, 0)
        group_hid = (group_act * up).astype(bf16)
        for k in group:
            lat[k] = cut(group_lat, k, group, 1)
            act[k] = cut(group_act, k, group, 0)
            hid[k] = cut(group_hid, k, group, 0)

    sums = jnp.zeros((2 * rank + 2, r * seq), bf16)
    grad_up_second, grad_down_first = [], []
    for group in [[k] for k in range(r)]:
        g = jnp.concatenate([grad_out[k] for k in group], axis=0)
        back = contract(down_adapter_second, g, 1, 1).astype(bf16)
        grad_hidden = matmul(g, down_weight) + adapter_scale * contract(back, down_first, 0, 1)
        grad_up = jnp.concatenate([act[k] for k in group], axis=0) * grad_hidden
        grad_up = grad_up.astype(bf16)
        up_lat = contract(up_second, grad_up, 1, 1)
        for k in group:
            grad_down_first.append(adapter_scale * matmul(cut(back, k, group, 1), hid[k]))
            grad_up_second.append(adapter_scale * matmul(lat[k], cut(grad_up, k, group, 0)))
            split = square(grad_down_first[k]) + square(grad_up_second[k])
            high = split.astype(bf16)
            low = (split - high.astype(f32)).astype(bf16)
            partial = [
                contract(down_first, hid[k], 0, 1).astype(bf16),
                cut(up_lat, k, group, 1).astype(bf16),
                jnp.broadcast_to(high, (1, seq)),
                jnp.broadcast_to(low, (1, seq)),
            ]
            partial = jnp.concatenate(partial, axis=0)
            sums = lax.dynamic_update_slice(sums, partial, (0, places[k] * seq))

    products = []
    for tokens in (grad_out, normed):
        for t in tokens:
            products.append(contract(t, t, 1, 1))
    products = jnp.stack(lax.optimization_barrier(products))
    share = lambda t: lax.dynamic_slice(t, (0, o * p * block), (seq, p * block))
    grad_share = jnp.concatenate([share(g) for g in grad_out], axis=0)
    normed_share = jnp.concatenate([share(n) for n in normed], axis=0)

    sums = jnp.sum(lax.all_gather(sums, ("o", "mp"), axis=0).astype(f32), axis=0)
    sums = jnp.concatenate(
        [lax.dynamic_slice(sums, (0, places[k] * seq), (2 * rank + 2, seq)) for k in range(r)], axis=1
    )
    lat_down = sums[:rank].astype(bf16).astype(f32)
    up_lat = sums[rank : 2 * rank].astype(bf16).astype(f32)
    latents = jnp.concatenate([lat_down, up_lat], axis=1).reshape(rank, 2 * r, seq).swapaxes(0, 1)
    through = lax.dot_general(
        latents, products, (((2,), (1,)), ((0,), (0,))), precision=lax.Precision.HIGHEST
    )
    squares = adapter_scale**2 * jnp.sum(latents * through, axis=(1, 2)).reshape(2, r).sum(axis=0)
    squares = squares + sums[2 * rank, ::seq] + sums[2 * rank + 1, ::seq]
    factors = jnp.minimum(1.0, clip_limit / (jnp.sqrt(squares) + 1e-06))

    def clipped(arrays):
        return sum(factors[k] * array for k, array in enumerate(arrays))

    by_token = jnp.repeat(adapter_scale * factors, seq)[None]

    def token_gradient(latent, tokens):
        scaled = by_token * latent
        high = scaled.astype(bf16)
        low = (scaled - high.astype(f32)).astype(bf16)
        both = matmul(jnp.concatenate([high, low], axis=0), tokens)
        return both[:rank] + both[rank:]

    sizes = (block, hidden // p, hidden // p, block)
    pieces = (
        token_gradient(up_lat, normed_share),
        clipped(grad_up_second),
        clipped(grad_down_first),
        token_gradient(lat_down, grad_share),
    )
    pieces = [a.astype(bf16) for a in pieces]
    pieces = jnp.concatenate(
        [a[:, j * size : (j + 1) * size] for j in range(p) for a, size in zip(pieces, sizes)], axis=1
    )
    pieces = pieces.reshape(rank, p, -1).swapaxes(0, 1)
    total = lax.all_to_all(pieces, "i", 0, 0, tiled=True)
    total = jnp.sum(total.reshape(p, rank, -1).astype(f32), axis=0)
    outs, start = [], 0
    for size in sizes:
        outs.append(total[:, start : start + size])
        start += size
    return outs[0].T, outs[1], outs[2].T, outs[3]


def solution(mesh):
    dp, mp = mesh.shape["dp"], mesh.shape["mp"]
    r = outer_count(dp)
    p = dp // r
    grid = Mesh(mesh.devices.reshape(r, p, mp), ("o", "i", "mp"))
    rows = ("o", "i")

    def body(*args):
        return per_device(*args, r=r, p=p)

    return jax.shard_map(
        body,
        mesh=grid,
        in_specs=(
            P(rows, "mp"),
            P(rows, "mp"),
            P(rows),
            P(),
            P(rows, "mp"),
            P(rows, "mp"),
            P(rows, "mp"),
            P(),
            P(None, "mp"),
            P("mp", None),
            P(),
        ),
        out_specs=(P(rows, None), P(None, ("mp", "o", "i")), P(("mp", "o", "i"), None), P(None, rows)),
        check_vma=False,
    )
```
